32 devices in a mesh: dp: 4 (over z), tp: 8 (over y, x, core).
Axes of the slice: x: 2, y: 2, z: 4, core: 2. Of those that a mesh axis runs over, the one named last changes fastest.
Arguments:
- w_up: bfloat16 [2, 2560, 10240], P(None, None, 'tp')
- w_down: bfloat16 [2, 10240, 2560], P(None, 'tp')
- x_saved: bfloat16 [2, 4, 2048, 2560], P(None, 'dp')
- h_saved: bfloat16 [2, 4, 2048, 10240], P(None, 'dp', None, 'tp')
- grad_out: bfloat16 [4, 2048, 2560], P('dp')
Outputs:
- output 1: bfloat16 [4, 2048, 2560], P('dp')
- output 2: float32 [2, 2560, 10240], P(None, None, 'tp')
- output 3: float32 [2, 10240, 2560], P(None, 'tp')
All inputs are finite; a program needn't handle non-finite values.
Results may differ from the reference program's by a relative error of at most 0.0130839.
Values are sent between devices in bfloat16 or wider.
A program may use at most 1 GiB of HBM per device.

```python
import jax
import jax.numpy as jnp
from jax import lax

LAYER_COUNT = 2
BATCH_ALL = 4
SEQ_LEN = 2048
D = 2560
F = 10240


def gelu_parts(hidden):
    tanh_val = jnp.tanh(0.7978845608028654 * (hidden + 0.044715 * hidden * hidden * hidden))
    gelu_out = 0.5 * hidden * (1.0 + tanh_val)
    gelu_slope = 0.5 * (1.0 + tanh_val) + 0.5 * hidden * (1.0 - tanh_val * tanh_val) * 0.7978845608028654 * (1.0 + 0.134145 * hidden * hidden)
    return gelu_out, gelu_slope


def forward_saved(x_first, w_up, w_down):
    rows_cur = x_first.reshape(BATCH_ALL * SEQ_LEN, D)
    x_list = []
    h_list = []
    for layer_idx in range(LAYER_COUNT):
        hidden = jnp.dot(rows_cur, w_up[layer_idx], preferred_element_type=jnp.float32).astype(jnp.bfloat16)
        gelu_out = gelu_parts(hidden.astype(jnp.float32))[0]
        branch = jnp.dot(gelu_out.astype(jnp.bfloat16), w_down[layer_idx], preferred_element_type=jnp.float32)
        x_list.append(rows_cur)
        h_list.append(hidden)
        rows_cur = (rows_cur.astype(jnp.float32) + branch).astype(jnp.bfloat16)
    x_saved = jnp.stack(x_list).reshape(LAYER_COUNT, BATCH_ALL, SEQ_LEN, D)
    h_saved = jnp.stack(h_list).reshape(LAYER_COUNT, BATCH_ALL, SEQ_LEN, F)
    return x_saved, h_saved


def setup_inputs(seed: int = 0) -> dict:
    root_key = jax.random.key(seed)
    key_x, key_up, key_down, key_grad = jax.random.split(root_key, 4)
    x_first = jax.random.normal(key_x, (BATCH_ALL, SEQ_LEN, D), jnp.float32).astype(jnp.bfloat16)
    w_up = (jax.random.normal(key_up, (LAYER_COUNT, D, F), jnp.float32) * (D ** -0.5)).astype(jnp.bfloat16)
    w_down = (jax.random.normal(key_down, (LAYER_COUNT, F, D), jnp.float32) * (F ** -0.5)).astype(jnp.bfloat16)
    grad_out = jax.random.normal(key_grad, (BATCH_ALL, SEQ_LEN, D), jnp.float32).astype(jnp.bfloat16)
    x_saved, h_saved = forward_saved(x_first, w_up, w_down)
    return {"w_up": w_up, "w_down": w_down, "x_saved": x_saved, "h_saved": h_saved, "grad_out": grad_out}


def reference(w_up, w_down, x_saved, h_saved, grad_out):
    def one_sequence(accums, seq_idx):
        up_acc, down_acc = accums
        grad_cur = grad_out[seq_idx]
        up_new = [None] * LAYER_COUNT
        down_new = [None] * LAYER_COUNT
        for layer_idx in reversed(range(LAYER_COUNT)):
            x_seq = x_saved[layer_idx, seq_idx]
            gelu_out, gelu_slope = gelu_parts(h_saved[layer_idx, seq_idx].astype(jnp.float32))
            act_grad = jnp.dot(grad_cur, w_down[layer_idx].T, preferred_element_type=jnp.float32)
            hid_grad = (act_grad * gelu_slope).astype(jnp.bfloat16)
            part_sum = jnp.dot(hid_grad, w_up[layer_idx].T, preferred_element_type=jnp.float32)
            down_new[layer_idx] = jnp.dot(gelu_out.astype(jnp.bfloat16).T, grad_cur, preferred_element_type=jnp.float32)
            up_new[layer_idx] = jnp.dot(x_seq.T, hid_grad, preferred_element_type=jnp.float32)
            grad_cur = (grad_cur.astype(jnp.float32) + part_sum).astype(jnp.bfloat16)
        return (up_acc + jnp.stack(up_new), down_acc + jnp.stack(down_new)), grad_cur
    zero_acc = (jnp.zeros((LAYER_COUNT, D, F), jnp.float32), jnp.zeros((LAYER_COUNT, F, D), jnp.float32))
    (up_grad, down_grad), grad_in = lax.scan(one_sequence, zero_acc, jnp.arange(BATCH_ALL))
    return grad_in, up_grad, down_grad
```

```python
import jax
import jax.numpy as jnp
from jax import lax
from jax.sharding import PartitionSpec as P


BF = jnp.bfloat16
F32 = jnp.float32


def gelu_parts(hidden):
    tanh_val = jnp.tanh(0.7978845608028654 * (hidden + 0.044715 * hidden * hidden * hidden))
    gelu_out = 0.5 * hidden * (1.0 + tanh_val)
    gelu_slope = 0.5 * (1.0 + tanh_val) + 0.5 * hidden * (1.0 - tanh_val * tanh_val) * 0.7978845608028654 * (1.0 + 0.134145 * hidden * hidden)
    return gelu_out, gelu_slope


def dot_nn(a, b):
    return lax.dot_general(a, b, (((1,), (0,)), ((), ())), preferred_element_type=F32)


def dot_nt(a, b):
    return lax.dot_general(a, b, (((1,), (1,)), ((), ())), preferred_element_type=F32)


def dot_tn(a, b):
    return lax.dot_general(a, b, (((0,), (0,)), ((), ())), preferred_element_type=F32)


def solution(mesh):
    n_dp, n_tp = mesh.shape["dp"], mesh.shape["tp"]

    def z_shift(v, k):
        return lax.ppermute(v, "dp", [(i, (i + k) % n_dp) for i in range(n_dp)])

    def flip(v, mask):
        return lax.ppermute(v, "tp", [(i, i ^ mask) for i in range(n_tp)])

    def plane_gather(v, x_first):
        if x_first:
            sx = flip(v, 2)
            sy = flip(v, 4)
            sxy = flip(sx, 4)
        else:
            sy = flip(v, 4)
            sx = flip(v, 2)
            sxy = flip(sy, 2)
        mine = [v, sx, sy, sxy]
        return jnp.concatenate(mine + [flip(s, 1) for s in mine], axis=0)

    def run_backward(w_up, w_down, x_saved, h_saved, grad_out):
        rows = x_saved.shape[2]
        part = rows // n_tp
        tp_idx = lax.axis_index("tp")

        def own_slice(v):
            return lax.dynamic_slice_in_dim(v, tp_idx * part, part, axis=0)

        x0, x1 = x_saved[0, 0], x_saved[1, 0]
        g2 = grad_out[0]

        def block_own(l, g):
            gelu_out, slope = gelu_parts(h_saved[l, 0].astype(F32))
            d_h = (dot_nt(g, w_down[l]) * slope).astype(BF)
            p = dot_nn(d_h, w_up[l].T).astype(BF)
            return gelu_out.astype(BF), d_h, p

        def block_other(l, x, g):
            h = dot_nn(x, w_up[l]).astype(BF)
            gelu_out, slope = gelu_parts(h.astype(F32))
            d_h = (dot_nt(g, w_down[l]) * slope).astype(BF)
            return gelu_out.astype(BF), d_h

        act, d_h, p1 = block_own(1, g2)
        p1_slice = lax.psum_scatter(p1, "tp", scatter_dimension=0, tiled=True)
        g1_slice = (own_slice(g2).astype(F32) + p1_slice.astype(F32)).astype(BF)
        g1_all = lax.all_gather(g1_slice, ("dp", "tp"), axis=0, tiled=True)

        up1 = dot_tn(x1, d_h)
        down1 = dot_tn(act, g2)
        x1s, g2s = own_slice(x1), own_slice(g2)
        for k in range(1, n_dp):
            xk = plane_gather(z_shift(x1s, k), True)
            gk = plane_gather(z_shift(g2s, k), False)
            act, d_h = block_other(1, xk, gk)
            up1 = up1 + dot_tn(xk, d_h)
            down1 = down1 + dot_tn(act, gk)

        dp_idx = lax.axis_index("dp")
        g1 = lax.dynamic_slice_in_dim(g1_all, dp_idx * rows, rows, axis=0)
        _, _, p0 = block_own(0, g1)
        x0s, _ = lax.optimization_barrier((own_slice(x0), g1_slice))
        x0_all = lax.all_gather(x0s, ("dp", "tp"), axis=0, tiled=True)
        sum0 = lax.psum(p0, "tp")
        g0 = (g1.astype(F32) + sum0.astype(F32)).astype(BF)
        act, d_h = block_other(0, x0_all, g1_all)
        up0 = dot_tn(x0_all, d_h)
        down0 = dot_tn(act, g1_all)
        return g0[None], jnp.stack([up0, up1]), jnp.stack([down0, down1])

    return jax.shard_map(run_backward, mesh=mesh, in_specs=(P(None, None, "tp"), P(None, "tp", None), P(None, "dp", None, None), P(None, "dp", None, "tp"), P("dp", None, None)), out_specs=(P("dp", None, None), P(None, None, "tp"), P(None, "tp", None)), check_vma=False)
```

```python
import functools

import jax
import jax.numpy as jnp
from jax import lax
from jax.experimental import pallas as pl
from jax.experimental.pallas import tpu as pltpu
from jax.sharding import PartitionSpec as P

BF = jnp.bfloat16
F32 = jnp.float32
MESH = pl.DeviceIdType.MESH

N_DP = 4
N_TP = 8
def gelu_parts(hidden):
    sq = hidden * hidden
    tanh_val = jnp.tanh(0.7978845608028654 * (hidden + 0.044715 * sq * hidden))
    gelu_out = 0.5 * hidden * (1.0 + tanh_val)
    gelu_slope = 0.5 * (1.0 + tanh_val) + 0.5 * hidden * (1.0 - tanh_val * tanh_val) * 0.7978845608028654 * (1.0 + 0.134145 * sq)
    return gelu_out, gelu_slope


def dot_nn(a, b):
    return lax.dot_general(a, b, (((1,), (0,)), ((), ())), preferred_element_type=F32)


def dot_nt(a, b):
    return lax.dot_general(a, b, (((1,), (1,)), ((), ())), preferred_element_type=F32)


def dot_tn(a, b):
    return lax.dot_general(a, b, (((0,), (0,)), ((), ())), preferred_element_type=F32)


OWN = 4
HALF = 16
STEPS = 2 * HALF
ROUTES = {
    (1, 0, 0): ("", (1, 1, 4, 15)),
    (1, 0, 1): ("dx", (1, 7, 10, 8)),
    (1, 1, 0): ("dx", (5, 12, 11, 7)),
    (1, 1, 1): ("x", (1, 8, 4, 16)),
    (1, 2, 0): ("d", (11, 28, 22, 49)),
    (1, 2, 1): ("dx", (31, 38, 44, 44)),
    (1, 3, 1): ("x", (-1, 45, 45, 59)),
    (0, 0, 0): ("dx", (37, 75, 55, 25)),
    (0, 0, 1): ("", (51, 70, 69, 78)),
    (0, 1, 0): ("dx", (65, 71, 89, 93)),
    (0, 1, 1): ("dx", (71, 93, 89, 76)),
    (0, 2, 0): ("dx", (55, 72, 72, 86)),
    (0, 2, 1): ("dx", (101, 110, 110, 108)),
    (0, 3, 1): ("x", (-1, 114, 122, 124)),
}
Z_ORDER = ((0, 0), (1, 0), (0, 6), (1, 6))
X0_TICKS = (17, 12)
REDUCE = {1: 34, 0: 106}
MASKS = (0, 2, 4, 6)


def events_by_tick():
    found = {}
    for (blk, slot, arr), (_, at) in ROUTES.items():
        for mask, tick in zip(MASKS, at):
            if tick >= 0:
                found.setdefault(tick, []).append((blk, slot, arr, mask))
    for evs in found.values():
        evs.sort(key=lambda ev: ((ev[3] + 2) // 4, -ev[0], ev[1:]))
    return sorted(found.items())


def kernel(*refs):
    (w_up, w_dn, x_sv, h_sv, g_in, g_out, dw1, dw2, xg, gg, rsr, pair,
     w1, w2, acc1, acc2, xb, gb, hb, ab, dhb, pst, pcb, misc, x_sem, g_sem, h_sem, rs_pc, rs_own, recv, send) = refs

    part = gb.shape[0] // 2
    dim, hid = w1.shape
    z = lax.axis_index("dp")
    p = lax.axis_index("tp")
    bit_c, bit_x, bit_y = p % 2, (p // 2) % 2, p // 4

    def ident(mask):
        out = p
        if mask & 1:
            out = out + 1 - 2 * bit_c
        if mask & 2:
            out = out + 2 - 4 * bit_x
        if mask & 4:
            out = out + 4 - 8 * bit_y
        return out

    def flipped(flip_y, flip_x, flip_c):
        return ((bit_y + flip_y) % 2) * 4 + ((bit_x + flip_x) % 2) * 2 + (bit_c + flip_c) % 2

    def rows(idx):
        return pl.ds(pl.multiple_of(idx * part, part), part)

    def buf_slice(blk, slot, arr, mask):
        if slot == 3:
            return g_out.at[blk, rows(ident(mask)), :]
        return (xg, gg)[arr].at[blk, slot, rows(ident(mask)), :]

    def recv_idx(blk, slot, arr, mask):
        return ((blk * 4 + slot) * 2 + arr) * 8 + mask

    sent = []

    def remote(src, dst, where, rsem, cond=None):
        idx = len(sent)

        def make():
            return pltpu.make_async_remote_copy(src_ref=src(), dst_ref=dst(), send_sem=send.at[idx], recv_sem=rsem(), device_id=where(), device_id_type=MESH)

        sent.append((make, cond))
        if cond is None:
            make().start()
        else:
            pl.when(cond())(lambda: make().start())

    def wait_on(here, sem):
        pltpu.make_async_copy(here, here, sem).wait()

    def wait_arrival(*ev):
        wait_on(buf_slice(*ev), recv.at[recv_idx(*ev)])

    def forward(blk, slot, arr, mask, flip):
        remote(lambda: buf_slice(blk, slot, arr, mask), lambda: buf_slice(blk, slot, arr, mask), lambda: (z, ident(flip)), lambda: recv.at[recv_idx(blk, slot, arr, mask ^ flip)])

    def direct(blk, slot, arr):
        return "d" in ROUTES[blk, slot, arr][0]

    def is_end():
        return z % 3 == 0

    def is_inner():
        return z % 3 != 0

    def toward_middle():
        return z + 1 - 2 * (z // 2)

    def toward_end():
        return (z - 1 + 2 * (z // 2)) % N_DP

    def z_copy(src, blk, slot, arr, mask, dest, cond):
        if mask == 0 or direct(blk, slot, arr):
            remote(src, lambda: buf_slice(blk, slot, arr, mask), lambda: (dest(), p), lambda: recv.at[recv_idx(blk, slot, arr, mask)], cond)

    def z_send(blk, arr, mask):
        def src():
            whole = x_sv.at[blk] if arr == 0 else (g_in if blk == 1 else g_out.at[1])
            return whole.at[rows(ident(mask)), :]

        z_copy(src, blk, 0, arr, mask, toward_end, is_inner)
        z_copy(src, blk, 0, arr, mask, toward_middle, is_end)
        z_copy(src, blk, 1, arr, mask, toward_middle, is_inner)

    def send_on(blk, slot, arr, mask):
        first, second = (2, 4) if "x" in ROUTES[blk, slot, arr][0] else (4, 2)
        if slot < 3 and mask in (0, 6):
            where = (2, toward_middle) if slot == 0 else (slot, toward_end)
            z_copy(lambda: buf_slice(blk, slot, arr, mask), blk, where[0], arr, mask, where[1], is_inner)
        if mask == 0:
            forward(blk, slot, arr, 0, first)
            forward(blk, slot, arr, 0, second)
        elif mask == first and not direct(blk, slot, arr):
            forward(blk, slot, arr, first, second)
        forward(blk, slot, arr, mask, 1)
        if (blk, slot, mask) == (1, 3, 6):
            z_send(0, 1, 6)

    def halves(half):
        return pl.ds(half * part, part)

    def fetch(arr, step, dst, sem):
        at = step % HALF
        blk = 1 - step // HALF

        @pl.when(at < OWN)
        def _():
            for half in range(2):
                idx = flipped(at // 2, at % 2, half)
                if arr == 0:
                    pltpu.make_async_copy(x_sv.at[blk, rows(idx), :], dst(half), sem(half)).start()
                else:
                    @pl.when(blk == 1)
                    def _():
                        pltpu.make_async_copy(g_in.at[rows(idx), :], dst(half), sem(half)).start()

                    @pl.when(blk == 0)
                    def _():
                        here = g_out.at[1, rows(idx), :]
                        if half == 1:
                            wait_on(here, recv.at[recv_idx(1, 3, 1, 2 * at + 1)])
                        pltpu.make_async_copy(here, dst(half), sem(half)).start()

        @pl.when(at >= OWN)
        def _():
            slot = (at - OWN) // 4
            quarter = (at - OWN) % 4
            buf = (xg, gg)[arr]
            for half in range(2):
                here = buf.at[blk, slot, rows(flipped(quarter % 2, half, quarter // 2)), :]

                @pl.when(quarter >= 2)
                def _():
                    wait_on(here, recv.at[recv_idx(blk, slot, arr, 1 + 4 * (quarter % 2) + 2 * half)])

                pltpu.make_async_copy(here, dst(half), sem(half)).start()

    def x_dst(step):
        slot = step % 2
        return (lambda half: xb.at[slot, halves(half), :]), (lambda half: x_sem.at[slot * 2 + half])

    def g_dst():
        return (lambda half: gb.at[halves(half), :]), (lambda half: g_sem.at[half])

    def fetched(dst, sem):
        for half in range(2):
            wait_on(dst(half), sem(half))

    def h_fetch(step):
        at = step % HALF
        for half in range(2):
            pltpu.make_async_copy(h_sv.at[1 - step // HALF, rows(flipped(at // 2, at % 2, half)), :], hb.at[halves(half), :], h_sem.at[half]).start()

    def pair_copy(blk, at):
        return pltpu.make_async_remote_copy(src_ref=pst.at[halves(1), :], dst_ref=pcb.at[at % 2], send_sem=misc.at[0], recv_sem=rs_pc.at[blk * OWN + at], device_id=(z, ident(1)), device_id_type=MESH)

    chunk = 16

    def pair_sum(blk, at):
        wait_on(pcb.at[at % 2], rs_pc.at[blk * OWN + at])
        pair_copy(blk, at).wait_send()

        def add(r, carry):
            where = pl.ds(pl.multiple_of(r * chunk, chunk), chunk)
            pst[where, :] = (pst[where, :].astype(F32) + pcb[at % 2, where, :].astype(F32)).astype(BF)
            return carry

        lax.fori_loop(0, part // chunk, add, 0)
        copy = pltpu.make_async_copy(pst.at[halves(0), :], pair.at[blk, at], misc.at[1])
        copy.start()
        copy.wait()
        if at:
            remote(lambda: pair.at[blk, at], lambda: rsr.at[blk, at - 1], lambda: (z, ident(2 * at)), lambda: rs_own.at[blk * 3 + at - 1])

    def reduce_own(blk):
        for s in range(3):
            wait_on(rsr.at[blk, s], rs_own.at[blk * 3 + s])
        before = g_in if blk == 1 else g_out.at[1]
        loads = [
            pltpu.make_async_copy(pair.at[blk, 0], pst.at[halves(0), :], misc.at[1]),
            pltpu.make_async_copy(rsr.at[blk, 0], pst.at[halves(1), :], misc.at[2]),
            pltpu.make_async_copy(rsr.at[blk, 1], pcb.at[0], misc.at[3]),
            pltpu.make_async_copy(rsr.at[blk, 2], pcb.at[1], misc.at[4]),
            pltpu.make_async_copy(before.at[rows(p), :], gb.at[halves(0), :], misc.at[5]),
        ]
        for load in loads:
            load.start()
        for load in loads:
            load.wait()

        def add(r, carry):
            lo = pl.ds(pl.multiple_of(r * chunk, chunk), chunk)
            hi = pl.ds(pl.multiple_of(part + r * chunk, chunk), chunk)
            total = (pst[lo, :].astype(F32) + pst[hi, :].astype(F32)) + (pcb[0, lo, :].astype(F32) + pcb[1, lo, :].astype(F32))
            pst[lo, :] = (gb[lo, :].astype(F32) + total).astype(BF)
            return carry

        lax.fori_loop(0, part // chunk, add, 0)
        copy = pltpu.make_async_copy(pst.at[halves(0), :], g_out.at[blk, rows(p), :], misc.at[1])
        copy.start()
        copy.wait()
        send_on(blk, 3, 1, 0)
        if blk == 1:
            z_send(0, 1, 0)

    def ticks(step, point):
        for blk in (1, 0):
            if REDUCE[blk] % 4 == point:
                pl.when(step == REDUCE[blk] // 4)(functools.partial(reduce_own, blk))
        for mask, tick in zip((0, 6), X0_TICKS):
            if tick % 4 == point:
                pl.when(step == tick // 4)(functools.partial(z_send, 0, 0, mask))
        for tick, evs in events_by_tick():
            if tick % 4 == point:
                @pl.when(step == tick // 4)
                def _(evs=evs):
                    for ev in evs:
                        wait_arrival(*ev)
                        send_on(*ev)

    def load_w1(blk):
        return pltpu.make_async_copy(w_up.at[blk], w1, misc.at[2])

    def load_w2(blk):
        return pltpu.make_async_copy(w_dn.at[blk], w2, misc.at[3])

    def store_1(blk):
        return pltpu.make_async_copy(acc1, dw1.at[blk], misc.at[4])

    def store_2(blk):
        return pltpu.make_async_copy(acc2, dw2.at[blk], misc.at[5])

    def clear(ref):
        def some(r, carry):
            ref[pl.ds(pl.multiple_of(r * 16, 16), 16), :] = jnp.zeros((16, ref.shape[1]), F32)
            return carry

        lax.fori_loop(0, ref.shape[0] // 16, some, 0)

    load_w2(1).start()
    fetch(1, 0, *g_dst())
    h_fetch(0)
    fetch(0, 0, *x_dst(0))
    load_w1(1).start()
    for arr, mask in Z_ORDER:
        z_send(1, arr, mask)
    clear(acc2)
    clear(acc1)
    load_w2(1).wait()
    load_w1(1).wait()

    n_hid = 256
    n_dim = 512

    def hid_cols(j):
        return pl.ds(pl.multiple_of(j * n_hid, n_hid), n_hid)

    def dim_cols(j):
        return pl.ds(pl.multiple_of(j * n_dim, n_dim), n_dim)

    def step_body(step, carry):
        slot = step % 2
        at = step % HALF
        is_own = at < OWN
        ticks(step, 0)
        fetched(*x_dst(step))

        @pl.when(is_own)
        def _():
            for half in range(2):
                wait_on(hb.at[halves(half), :], h_sem.at[half])

        @pl.when(at >= OWN)
        def _():
            def h_part(j, c):
                hb[:, hid_cols(j)] = dot_nn(xb[slot], w1[:, hid_cols(j)]).astype(BF)
                return c

            lax.fori_loop(0, hid // n_hid, h_part, 0, unroll=True)

        ticks(step, 1)

        @pl.when(step == HALF - 1)
        def _():
            load_w1(0).start()

        @pl.when(step == HALF)
        def _():
            store_2(1).wait()
            clear(acc2)
            load_w2(0).wait()

        fetched(*g_dst())

        def a_part(j, c):
            act, slope = gelu_parts(hb[:, hid_cols(j)].astype(F32))
            ab[:, hid_cols(j)] = act.astype(BF)
            dhb[:, hid_cols(j)] = (dot_nt(gb[...], w2[hid_cols(j), :]) * slope).astype(BF)
            return c

        lax.fori_loop(0, hid // n_hid, a_part, 0, unroll=True)

        def down_part(j, c):
            acc2[hid_cols(j), :] += dot_tn(ab[:, hid_cols(j)], gb[...])
            return c

        lax.fori_loop(0, hid // n_hid, down_part, 0, unroll=True)

        @pl.when(step == HALF - 1)
        def _():
            load_w2(0).start()
            store_2(1).start()

        ticks(step, 2)

        @pl.when(step + 1 < STEPS)
        def _():
            fetch(0, step + 1, *x_dst(step + 1))
            fetch(1, step + 1, *g_dst())

        @pl.when((step + 1) % HALF < OWN)
        def _():
            pl.when(step + 1 < STEPS)(lambda: h_fetch(step + 1))

        for blk in (1, 0):
            for b in range(OWN):
                pl.when(step == (1 - blk) * HALF + b + 1)(functools.partial(pair_sum, blk, b))

        @pl.when(step == HALF)
        def _():
            load_w1(0).wait()

        @pl.when(is_own)
        def _():
            def p_part(j, c):
                pst[:, dim_cols(j)] = dot_nt(dhb[...], w1[dim_cols(j), :]).astype(BF)
                return c

            lax.fori_loop(0, dim // n_dim, p_part, 0, unroll=True)

        ticks(step, 3)
        for blk in (1, 0):
            for b in range(OWN):
                pl.when(step == (1 - blk) * HALF + b)(lambda blk=blk, b=b: pair_copy(blk, b).start())

        @pl.when(step == HALF)
        def _():
            store_1(1).wait()
            clear(acc1)

        def up_part(j, c):
            acc1[dim_cols(j), :] += dot_tn(xb[slot, :, dim_cols(j)], dhb[...])
            return c

        lax.fori_loop(0, dim // n_dim, up_part, 0, unroll=True)

        @pl.when(step == HALF - 1)
        def _():
            store_1(1).start()

        return carry

    lax.fori_loop(0, STEPS, step_body, 0)

    store_2(0).start()
    store_1(0).start()
    for mask in (1, 3, 5, 7):
        wait_arrival(0, 3, 1, mask)
    for make, cond in sent:
        if cond is None:
            make().wait_send()
        else:
            pl.when(cond())(lambda make=make: make().wait_send())
    store_2(0).wait()
    store_1(0).wait()


def backward(w_up, w_dn, x_sv, h_sv, g_in):
    _, dim, hid = w_up.shape
    tokens = g_in.shape[0]
    part = tokens // N_TP
    hbm = pl.BlockSpec(memory_space=pl.ANY)
    outs = [
        jax.ShapeDtypeStruct((2, tokens, dim), BF),
        jax.ShapeDtypeStruct((2, dim, hid), F32),
        jax.ShapeDtypeStruct((2, hid, dim), F32),
        jax.ShapeDtypeStruct((2, 3, tokens, dim), BF),
        jax.ShapeDtypeStruct((2, 3, tokens, dim), BF),
        jax.ShapeDtypeStruct((2, 3, part, dim), BF),
        jax.ShapeDtypeStruct((2, 4, part, dim), BF),
    ]
    dma = pltpu.SemaphoreType.DMA
    scratch = [
        pltpu.VMEM((dim, hid), BF),
        pltpu.VMEM((hid, dim), BF),
        pltpu.VMEM((dim, hid), F32),
        pltpu.VMEM((hid, dim), F32),
        pltpu.VMEM((2, 2 * part, dim), BF),
        pltpu.VMEM((2 * part, dim), BF),
        pltpu.VMEM((2 * part, hid), BF),
        pltpu.VMEM((2 * part, hid), BF),
        pltpu.VMEM((2 * part, hid), BF),
        pltpu.VMEM((2 * part, dim), BF),
        pltpu.VMEM((2, part, dim), BF),
        dma((6,)),
        dma((4,)),
        dma((2,)),
        dma((2,)),
        dma((2 * OWN,)),
        dma((6,)),
        dma((128,)),
        dma((176,)),
    ]
    return pl.pallas_call(
        kernel,
        out_shape=outs,
        in_specs=[hbm] * 5,
        out_specs=[hbm] * len(outs),
        scratch_shapes=scratch,
        compiler_params=pltpu.CompilerParams(has_side_effects=True, vmem_limit_bytes=67043328),
        cost_estimate=pl.CostEstimate(flops=STEPS * 4 * 4 * part * dim * hid, bytes_accessed=0, transcendentals=0),
        name="backward",
    )(w_up, w_dn, x_sv, h_sv, g_in)


def solution(mesh):
    def run_backward(w_up, w_down, x_saved, h_saved, grad_out):
        grads, up, down, *_ = backward(w_up, w_down, x_saved[:, 0], h_saved[:, 0], grad_out[0])
        return grads[:1], up, down

    return jax.shard_map(run_backward, mesh=mesh, in_specs=(P(None, None, "tp"), P(None, "tp", None), P(None, "dp", None, None), P(None, "dp", None, "tp"), P("dp", None, None)), out_specs=(P("dp", None, None), P(None, None, "tp"), P(None, "tp", None)), check_vma=False)
```

```python
import functools

import jax
import jax.numpy as jnp
from jax import lax
from jax.experimental import pallas as pl
from jax.experimental.pallas import tpu as pltpu
from jax.sharding import PartitionSpec as P

BF = jnp.bfloat16
F32 = jnp.float32
MESH = pl.DeviceIdType.MESH

N_DP = 4
N_TP = 8
def gelu_parts(hidden):
    sq = hidden * hidden
    tanh_val = jnp.tanh(0.7978845608028654 * (hidden + 0.044715 * sq * hidden))
    gelu_out = 0.5 * hidden * (1.0 + tanh_val)
    gelu_slope = 0.5 * (1.0 + tanh_val) + 0.5 * hidden * (1.0 - tanh_val * tanh_val) * 0.7978845608028654 * (1.0 + 0.134145 * sq)
    return gelu_out, gelu_slope


def dot_nn(a, b):
    return lax.dot_general(a, b, (((1,), (0,)), ((), ())), preferred_element_type=F32)


def dot_nt(a, b):
    return lax.dot_general(a, b, (((1,), (1,)), ((), ())), preferred_element_type=F32)


def dot_tn(a, b):
    return lax.dot_general(a, b, (((0,), (0,)), ((), ())), preferred_element_type=F32)


OWN = 4
HALF = 16
STEPS = 2 * HALF
SUB = 2
KEYS = [(blk, slot, arr) for blk in (1, 0) for slot in range(4) for arr in range(2) if slot < 3 or arr == 1]
ROUTES = (
    ("x", "0103040d090c1214"),
    ("dx", "0407080d0a100d14"),
    ("dx", "0d151c1c17220f19"),
    ("", "0c1114160d1b1522"),
    ("d", "0e21162a162b3136"),
    ("d", "152a2c2e2d2f2c35"),
    ("x", "00002d2e2f324447"),
    ("", "2d34323e3748434d"),
    ("dx", "2e2e363a41454c51"),
    ("dx", "3a514b5d565c435d"),
    ("x", "3f52495a4c5b5366"),
    ("d", "5769696e64726470"),
    ("dx", "4d5f526953736b76"),
    ("", "0000717d73777c7d"),
)
Z_ORDER = ((0, 0), (1, 0), (0, 6), (1, 6))
X0_TICKS = (27, 4)
COMBINE = {1: 26, 0: 94}
REDUCE = {1: 34, 0: 106}
ROUTE = dict(zip(KEYS, ROUTES))
PARTS = [(mask, sub) for mask in (0, 2, 4, 6) for sub in range(SUB)]


def events_by_tick():
    found = {}
    for (blk, slot, arr), (_, at) in ROUTE.items():
        for (mask, sub), tick in zip(PARTS, bytes.fromhex(at)):
            if slot < 3 or mask:
                found.setdefault(tick, []).append((blk, slot, arr, mask, sub))
    for evs in found.values():
        evs.sort(key=lambda ev: ((ev[3] + 2) // 4, -ev[0], ev[1:]))
    return sorted(found.items())


def kernel(*refs):
    (w_up, w_dn, x_sv, h_sv, g_in, g_0, g_1, dw1, dw2, xg, gg, rsr, pair,
     w1, w2, acc1, acc2, xb, gb, hb, ab, dhb, pst, pcb, misc, x_sem, g_sem, h_sem, rs_pc, rs_own, recv, send) = refs

    part = gb.shape[0] // 2
    small = part // SUB
    dim, hid = w1.shape
    g_out = (g_0, g_1)
    z = lax.axis_index("dp")
    p = lax.axis_index("tp")
    bit_c, bit_x, bit_y = p % 2, (p // 2) % 2, p // 4

    def ident(mask):
        out = p
        if mask & 1:
            out = out + 1 - 2 * bit_c
        if mask & 2:
            out = out + 2 - 4 * bit_x
        if mask & 4:
            out = out + 4 - 8 * bit_y
        return out

    def flipped(flip_y, flip_x, flip_c):
        return ((bit_y + flip_y) % 2) * 4 + ((bit_x + flip_x) % 2) * 2 + (bit_c + flip_c) % 2

    def rows(idx):
        return pl.ds(pl.multiple_of(idx * part, part), part)

    def sub_rows(idx, sub):
        return pl.ds(pl.multiple_of(idx * part + sub * small, small), small)

    def slice_at(blk, slot, arr, where):
        if slot == 3:
            return g_out[blk].at[where, :]
        return (xg, gg)[arr].at[blk, slot, where, :]

    def buf_part(blk, slot, arr, mask, sub):
        return slice_at(blk, slot, arr, sub_rows(ident(mask), sub))

    def buf_slice(blk, slot, arr, mask):
        return slice_at(blk, slot, arr, rows(ident(mask)))

    def recv_at(blk, slot, arr, mask, sub=0):
        return recv.at[(((blk * 4 + slot) * 2 + arr) * 8 + mask) * SUB + sub]

    sent = []

    def remote(src, dst, where, rsem, cond=None):
        idx = len(sent)

        def make():
            return pltpu.make_async_remote_copy(src_ref=src(), dst_ref=dst(), send_sem=send.at[idx], recv_sem=rsem(), device_id=where(), device_id_type=MESH)

        sent.append((make, cond))
        if cond is None:
            make().start()
        else:
            pl.when(cond())(lambda: make().start())

    def wait_on(here, sem):
        pltpu.make_async_copy(here, here, sem).wait()

    def forward(blk, slot, arr, mask, sub, flip):
        here = lambda: buf_part(blk, slot, arr, mask, sub)
        remote(here, here, lambda: (z, ident(flip)), lambda: recv_at(blk, slot, arr, mask ^ flip, sub))

    def to_partner(blk, slot, arr, mask):
        here = lambda: buf_slice(blk, slot, arr, mask)
        remote(here, here, lambda: (z, ident(1)), lambda: recv_at(blk, slot, arr, mask ^ 1))

    def direct(blk, slot, arr):
        return "d" in ROUTE[blk, slot, arr][0]

    def is_end():
        return z % 3 == 0

    def is_inner():
        return z % 3 != 0

    def toward_middle():
        return z + 1 - 2 * (z // 2)

    def toward_end():
        return (z - 1 + 2 * (z // 2)) % N_DP

    def z_copy(src, blk, slot, arr, mask, sub, dest, cond):
        if mask == 0 or direct(blk, slot, arr):
            remote(src, lambda: buf_part(blk, slot, arr, mask, sub), lambda: (dest(), p), lambda: recv_at(blk, slot, arr, mask, sub), cond)

    def z_send(blk, arr, mask, sub):
        def src():
            whole = x_sv.at[blk] if arr == 0 else (g_in if blk == 1 else g_1)
            return whole.at[sub_rows(ident(mask), sub), :]

        z_copy(src, blk, 0, arr, mask, sub, toward_end, is_inner)
        z_copy(src, blk, 0, arr, mask, sub, toward_middle, is_end)
        z_copy(src, blk, 1, arr, mask, sub, toward_middle, is_inner)

    def send_on(blk, slot, arr, mask, sub):
        first, second = (2, 4) if "x" in ROUTE[blk, slot, arr][0] else (4, 2)
        if slot < 3 and mask in (0, 6):
            where = (2, toward_middle) if slot == 0 else (slot, toward_end)
            z_copy(lambda: buf_part(blk, slot, arr, mask, sub), blk, where[0], arr, mask, sub, where[1], is_inner)
        if mask == 0:
            forward(blk, slot, arr, 0, sub, first)
            forward(blk, slot, arr, 0, sub, second)
        elif mask == first and not direct(blk, slot, arr):
            forward(blk, slot, arr, first, sub, second)
        if sub == SUB - 1:
            to_partner(blk, slot, arr, mask)
        if (blk, slot, mask) == (1, 3, 6):
            z_send(0, 1, 6, sub)

    def halves(half):
        return pl.ds(half * part, part)

    def fetch(arr, step, dst, sem):
        at = step % HALF
        blk = 1 - step // HALF

        @pl.when(at < OWN)
        def _():
            for half in range(2):
                idx = flipped(at // 2, at % 2, half)
                if arr == 0:
                    pltpu.make_async_copy(x_sv.at[blk, rows(idx), :], dst(half), sem(half)).start()
                else:
                    @pl.when(blk == 1)
                    def _():
                        pltpu.make_async_copy(g_in.at[rows(idx), :], dst(half), sem(half)).start()

                    @pl.when(blk == 0)
                    def _():
                        here = g_1.at[rows(idx), :]
                        if half == 1:
                            wait_on(here, recv_at(1, 3, 1, 2 * at + 1))
                        pltpu.make_async_copy(here, dst(half), sem(half)).start()

        @pl.when(at >= OWN)
        def _():
            slot = (at - OWN) // 4
            quarter = (at - OWN) % 4
            buf = (xg, gg)[arr]
            for half in range(2):
                here = buf.at[blk, slot, rows(flipped(quarter // 2, half, quarter % 2)), :]

                @pl.when(quarter % 2 == 1)
                def _():
                    wait_on(here, recv_at(blk, slot, arr, 1 + 4 * (quarter // 2) + 2 * half))

                pltpu.make_async_copy(here, dst(half), sem(half)).start()

    def x_dst(step):
        slot = step % 2
        return (lambda half: xb.at[slot, halves(half), :]), (lambda half: x_sem.at[slot * 2 + half])

    def g_dst():
        return (lambda half: gb.at[halves(half), :]), (lambda half: g_sem.at[half])

    def fetched(dst, sem):
        for half in range(2):
            wait_on(dst(half), sem(half))

    def h_fetch(step):
        at = step % HALF
        for half in range(2):
            pltpu.make_async_copy(h_sv.at[1 - step // HALF, rows(flipped(at // 2, at % 2, half)), :], hb.at[halves(half), :], h_sem.at[half]).start()

    def pair_copy(blk, at):
        return pltpu.make_async_remote_copy(src_ref=pst.at[halves(1), :], dst_ref=pcb.at[at % 2], send_sem=misc.at[0], recv_sem=rs_pc.at[blk * OWN + at], device_id=(z, ident(1)), device_id_type=MESH)

    chunk = 16

    def pair_sum(blk, at):
        wait_on(pcb.at[at % 2], rs_pc.at[blk * OWN + at])
        pair_copy(blk, at).wait_send()

        def add(r, carry):
            where = pl.ds(pl.multiple_of(r * chunk, chunk), chunk)
            pst[where, :] = (pst[where, :].astype(F32) + pcb[at % 2, where, :].astype(F32)).astype(BF)
            return carry

        lax.fori_loop(0, part // chunk, add, 0)
        copy = pltpu.make_async_copy(pst.at[halves(0), :], pair.at[blk, at], misc.at[1])
        copy.start()
        copy.wait()
        if at == 1:
            p_send(blk, 1, 0, 0, 0)
        if at == 2:
            p_send(blk, 2, 1, 1, 1)
        if at == 3:
            p_send(blk, 3, 0, 2, 0)
            p_send(blk, 3, 1, 2, 1)

    def half_rows(low):
        return pl.ds(low * (part // 2), part // 2)

    def p_send(blk, src, low, dst, axis):
        remote(lambda: pair.at[blk, src, half_rows(low), :], lambda: rsr.at[blk, dst, half_rows(low), :], lambda: (z, ident(2 + 2 * axis)), lambda: rs_own.at[blk * 6 + dst * 2 + low])

    def p_wait(blk, dst):
        for low in range(2):
            wait_on(rsr.at[blk, dst, half_rows(low), :], rs_own.at[blk * 6 + dst * 2 + low])

    def run_copies(copies):
        for copy in copies:
            copy.start()
        for copy in copies:
            copy.wait()

    def combine(blk):
        p_wait(blk, 2)
        run_copies([
            pltpu.make_async_copy(pair.at[blk, 2, half_rows(0), :], pst.at[half_rows(0), :], misc.at[1]),
            pltpu.make_async_copy(pair.at[blk, 1, half_rows(1), :], pst.at[half_rows(1), :], misc.at[2]),
            pltpu.make_async_copy(rsr.at[blk, 2], pcb.at[0], misc.at[3]),
        ])

        def add(r, carry):
            lo = pl.ds(pl.multiple_of(r * chunk, chunk), chunk)
            pst[lo, :] = (pst[lo, :].astype(F32) + pcb[0, lo, :].astype(F32)).astype(BF)
            return carry

        lax.fori_loop(0, part // chunk, add, 0)
        run_copies([
            pltpu.make_async_copy(pst.at[half_rows(0), :], pair.at[blk, 2, half_rows(0), :], misc.at[1]),
            pltpu.make_async_copy(pst.at[half_rows(1), :], pair.at[blk, 1, half_rows(1), :], misc.at[2]),
        ])
        p_send(blk, 2, 0, 1, 1)
        p_send(blk, 1, 1, 0, 0)

    def reduce_own(blk):
        p_wait(blk, 0)
        p_wait(blk, 1)
        before = g_in if blk == 1 else g_1
        run_copies([
            pltpu.make_async_copy(pair.at[blk, 0], pst.at[halves(0), :], misc.at[1]),
            pltpu.make_async_copy(rsr.at[blk, 0], pst.at[halves(1), :], misc.at[2]),
            pltpu.make_async_copy(rsr.at[blk, 1], pcb.at[0], misc.at[3]),
            pltpu.make_async_copy(before.at[rows(p), :], gb.at[halves(0), :], misc.at[5]),
        ])

        def add(r, carry):
            lo = pl.ds(pl.multiple_of(r * chunk, chunk), chunk)
            hi = pl.ds(pl.multiple_of(part + r * chunk, chunk), chunk)
            total = pst[lo, :].astype(F32) + pst[hi, :].astype(F32) + pcb[0, lo, :].astype(F32)
            pst[lo, :] = (gb[lo, :].astype(F32) + total).astype(BF)
            return carry

        lax.fori_loop(0, part // chunk, add, 0)
        run_copies([pltpu.make_async_copy(pst.at[halves(0), :], g_out[blk].at[rows(p), :], misc.at[1])])
        for sub in range(SUB):
            send_on(blk, 3, 1, 0, sub)
        if blk == 1:
            for sub in range(SUB):
                z_send(0, 1, 0, sub)

    def ticks(step, point):
        for blk in (1, 0):
            for when, act in ((COMBINE, combine), (REDUCE, reduce_own)):
                if when[blk] % 4 == point:
                    pl.when(step == when[blk] // 4)(functools.partial(act, blk))
        for mask, tick in zip((0, 6), X0_TICKS):
            if tick % 4 == point:
                @pl.when(step == tick // 4)
                def _(mask=mask):
                    for sub in range(SUB):
                        z_send(0, 0, mask, sub)
        for tick, evs in events_by_tick():
            if tick % 4 == point:
                @pl.when(step == tick // 4)
                def _(evs=evs):
                    for ev in evs:
                        wait_on(buf_part(*ev), recv_at(*ev))
                        send_on(*ev)

    def load_w1(blk):
        return pltpu.make_async_copy(w_up.at[blk], w1, misc.at[2])

    def load_w2(blk):
        return pltpu.make_async_copy(w_dn.at[blk], w2, misc.at[3])

    def store_1(blk):
        return pltpu.make_async_copy(acc1, dw1.at[blk], misc.at[4])

    def store_2(blk):
        return pltpu.make_async_copy(acc2, dw2.at[blk], misc.at[5])

    def clear(ref):
        def some(r, carry):
            ref[pl.ds(pl.multiple_of(r * 16, 16), 16), :] = jnp.zeros((16, ref.shape[1]), F32)
            return carry

        lax.fori_loop(0, ref.shape[0] // 16, some, 0)

    load_w2(1).start()
    fetch(1, 0, *g_dst())
    h_fetch(0)
    fetch(0, 0, *x_dst(0))
    load_w1(1).start()
    for arr, mask in Z_ORDER:
        for sub in range(SUB):
            z_send(1, arr, mask, sub)
    clear(acc2)
    clear(acc1)
    load_w2(1).wait()
    load_w1(1).wait()

    n_hid = 256
    n_dim = 512

    def hid_cols(j):
        return pl.ds(pl.multiple_of(j * n_hid, n_hid), n_hid)

    def dim_cols(j):
        return pl.ds(pl.multiple_of(j * n_dim, n_dim), n_dim)

    def step_body(step, carry):
        slot = step % 2
        at = step % HALF
        is_own = at < OWN
        ticks(step, 0)
        fetched(*x_dst(step))

        @pl.when(is_own)
        def _():
            for half in range(2):
                wait_on(hb.at[halves(half), :], h_sem.at[half])

        ticks(step, 1)

        @pl.when(step == HALF)
        def _():
            store_2(1).wait()
            clear(acc2)
            load_w2(0).wait()

        fetched(*g_dst())

        def a_part(j):
            act, slope = gelu_parts(hb[:, hid_cols(j)].astype(F32))
            ab[:, hid_cols(j)] = act.astype(BF)
            dhb[:, hid_cols(j)] = (dot_nt(gb[...], w2[hid_cols(j), :]) * slope).astype(BF)


        def h_part(j):
            hb[:, hid_cols(j)] = dot_nn(xb[slot], w1[:, hid_cols(j)]).astype(BF)

        def down():
            acc2[...] += dot_tn(ab[...], gb[...])

        @pl.when(is_own)
        def _():
            for j in range(hid // n_hid):
                a_part(j)
            down()

        @pl.when(at >= OWN)
        def _():
            h_part(0)
            for j in range(hid // n_hid):
                if j + 1 < hid // n_hid:
                    h_part(j + 1)
                a_part(j)
            down()

        @pl.when(step == HALF - 1)
        def _():
            load_w2(0).start()
            load_w1(0).start()
            store_2(1).start()

        @pl.when(step == STEPS - 1)
        def _():
            store_2(0).start()

        ticks(step, 2)

        @pl.when(step + 1 < STEPS)
        def _():
            fetch(0, step + 1, *x_dst(step + 1))
            fetch(1, step + 1, *g_dst())

        @pl.when((step + 1) % HALF < OWN)
        def _():
            pl.when(step + 1 < STEPS)(lambda: h_fetch(step + 1))

        for blk in (1, 0):
            for b in range(OWN):
                pl.when(step == (1 - blk) * HALF + b + 1)(functools.partial(pair_sum, blk, b))

        @pl.when(step == HALF)
        def _():
            load_w1(0).wait()

        @pl.when(is_own)
        def _():
            def p_part(j, c):
                pst[:, dim_cols(j)] = dot_nt(dhb[...], w1[dim_cols(j), :]).astype(BF)
                return c

            lax.fori_loop(0, dim // n_dim, p_part, 0, unroll=True)

        ticks(step, 3)
        for blk in (1, 0):
            for b in range(OWN):
                pl.when(step == (1 - blk) * HALF + b)(lambda blk=blk, b=b: pair_copy(blk, b).start())

        @pl.when(step == HALF)
        def _():
            store_1(1).wait()
            clear(acc1)

        def up_part(j, c):
            acc1[dim_cols(j), :] += dot_tn(xb[slot, :, dim_cols(j)], dhb[...])
            return c

        @pl.when(step < STEPS - 1)
        def _():
            lax.fori_loop(0, dim // n_dim, up_part, 0, unroll=True)

        @pl.when(step == HALF - 1)
        def _():
            store_1(1).start()

        return carry

    lax.fori_loop(0, STEPS, step_body, 0)

    def last_part(j):
        return pltpu.make_async_copy(acc1.at[dim_cols(j), :], dw1.at[0, dim_cols(j), :], misc.at[4])

    def last_up(j, c):
        acc1[dim_cols(j), :] += dot_tn(xb[(STEPS - 1) % 2, :, dim_cols(j)], dhb[...])

        @pl.when(j > 0)
        def _():
            last_part(j - 1).wait()

        last_part(j).start()
        return c

    lax.fori_loop(0, dim // n_dim, last_up, 0)
    last_part(dim // n_dim - 1).wait()
    for mask in (1, 3, 5, 7):
        wait_on(buf_slice(0, 3, 1, mask), recv_at(0, 3, 1, mask))
    for make, cond in sent:
        if cond is None:
            make().wait_send()
        else:
            pl.when(cond())(lambda make=make: make().wait_send())
    store_2(0).wait()


def backward(w_up, w_dn, x_sv, h_sv, g_in):
    _, dim, hid = w_up.shape
    tokens = g_in.shape[0]
    part = tokens // N_TP
    hbm = pl.BlockSpec(memory_space=pl.ANY)
    outs = [
        jax.ShapeDtypeStruct((tokens, dim), BF),
        jax.ShapeDtypeStruct((tokens, dim), BF),
        jax.ShapeDtypeStruct((2, dim, hid), F32),
        jax.ShapeDtypeStruct((2, hid, dim), F32),
        jax.ShapeDtypeStruct((2, 3, tokens, dim), BF),
        jax.ShapeDtypeStruct((2, 3, tokens, dim), BF),
        jax.ShapeDtypeStruct((2, 3, part, dim), BF),
        jax.ShapeDtypeStruct((2, 4, part, dim), BF),
    ]
    dma = pltpu.SemaphoreType.DMA
    scratch = [
        pltpu.VMEM((dim, hid), BF),
        pltpu.VMEM((hid, dim), BF),
        pltpu.VMEM((dim, hid), F32),
        pltpu.VMEM((hid, dim), F32),
        pltpu.VMEM((2, 2 * part, dim), BF),
        pltpu.VMEM((2 * part, dim), BF),
        pltpu.VMEM((2 * part, hid), BF),
        pltpu.VMEM((2 * part, hid), BF),
        pltpu.VMEM((2 * part, hid), BF),
        pltpu.VMEM((2 * part, dim), BF),
        pltpu.VMEM((2, part, dim), BF),
        dma((6,)),
        dma((4,)),
        dma((2,)),
        dma((2,)),
        dma((2 * OWN,)),
        dma((12,)),
        dma((256,)),
        dma((288,)),
    ]
    return pl.pallas_call(
        kernel,
        out_shape=outs,
        in_specs=[hbm] * 5,
        out_specs=[hbm] * len(outs),
        scratch_shapes=scratch,
        compiler_params=pltpu.CompilerParams(has_side_effects=True, vmem_limit_bytes=67043328),
        cost_estimate=pl.CostEstimate(flops=STEPS * 4 * 4 * part * dim * hid, bytes_accessed=0, transcendentals=0),
        name="backward",
    )(w_up, w_dn, x_sv, h_sv, g_in)


def solution(mesh):
    def run_backward(w_up, w_down, x_saved, h_saved, grad_out):
        grad_in, _, up, down, *_ = backward(w_up, w_down, x_saved[:, 0], h_saved[:, 0], grad_out[0])
        return grad_in[None], up, down

    return jax.shard_map(run_backward, mesh=mesh, in_specs=(P(None, None, "tp"), P(None, "tp", None), P(None, "dp", None, None), P(None, "dp", None, "tp"), P("dp", None, None)), out_specs=(P("dp", None, None), P(None, None, "tp"), P(None, "tp", None)), check_vma=False)
```

```python
import functools

import jax
import jax.numpy as jnp
from jax import lax
from jax.experimental import pallas as pl
from jax.experimental.pallas import tpu as pltpu
from jax.sharding import PartitionSpec as P

BF = jnp.bfloat16
F32 = jnp.float32
MESH = pl.DeviceIdType.MESH

N_DP = 4
N_TP = 8
def gelu_parts(hidden):
    sq = hidden * hidden
    tanh_val = jnp.tanh(0.7978845608028654 * (hidden + 0.044715 * sq * hidden))
    gelu_out = 0.5 * hidden * (1.0 + tanh_val)
    gelu_slope = 0.5 * (1.0 + tanh_val) + 0.5 * hidden * (1.0 - tanh_val * tanh_val) * 0.7978845608028654 * (1.0 + 0.134145 * sq)
    return gelu_out, gelu_slope


def dot_nn(a, b):
    return lax.dot_general(a, b, (((1,), (0,)), ((), ())), preferred_element_type=F32)


def dot_nt(a, b):
    return lax.dot_general(a, b, (((1,), (1,)), ((), ())), preferred_element_type=F32)


def dot_tn(a, b):
    return lax.dot_general(a, b, (((0,), (0,)), ((), ())), preferred_element_type=F32)


OWN = 4
HALF = 16
STEPS = 2 * HALF
SUB = 2
KEYS = [(blk, slot, arr) for blk in (1, 0) for slot in range(4) for arr in range(2) if slot < 3 or arr == 1]
ROUTES = (
    ("x", "0003090b080a0f11"),
    ("d", "06080d0e0a160c0c"),
    ("dx", "0e121414191b121a"),
    ("", "0c120f16141c1b24"),
    ("dx", "0f1f1e2a1d243036"),
    ("d", "1829202e1e2f2d35"),
    ("x", "00002a2d2c3a4647"),
    ("", "2935363e3648404e"),
    ("d", "2d3a394640494f54"),
    ("d", "3a4f49574862425a"),
    ("x", "3e54485d4d654f66"),
    ("d", "5861626c6f716575"),
    ("d", "4c5e526852706972"),
    ("", "0000787c74787b7d"),
)
Z_ORDER = ((0, 6), (0, 0), (1, 0), (1, 6))
X0_TICKS = (29, 2)
COMBINE = {1: 30, 0: 94}
REDUCE = {1: 34, 0: 106}
ROUTE = dict(zip(KEYS, ROUTES))
PARTS = [(mask, sub) for mask in (0, 2, 4, 6) for sub in range(SUB)]


def events_by_tick():
    found = {}
    for (blk, slot, arr), (_, at) in ROUTE.items():
        for (mask, sub), tick in zip(PARTS, bytes.fromhex(at)):
            if slot < 3 or mask:
                found.setdefault(tick, []).append((blk, slot, arr, mask, sub))
    for evs in found.values():
        evs.sort(key=lambda ev: ((ev[3] + 2) // 4, -ev[0], ev[1:]))
    return sorted(found.items())


def kernel(*refs):
    (w_up, w_dn, x_sv, h_sv, g_in, g_0, g_1, dw1, dw2, xg, gg, rsr, pair,
     w1, w2, acc1, acc2, xb, gb, hb, ab, dhb, pst, pcb, misc, x_sem, g_sem, h_sem, rs_pc, rs_own, recv, send) = refs

    part = gb.shape[0] // 2
    small = part // SUB
    dim, hid = w1.shape
    g_out = (g_0, g_1)
    z = lax.axis_index("dp")
    p = lax.axis_index("tp")
    bit_c, bit_x, bit_y = p % 2, (p // 2) % 2, p // 4

    def ident(mask):
        out = p
        if mask & 1:
            out = out + 1 - 2 * bit_c
        if mask & 2:
            out = out + 2 - 4 * bit_x
        if mask & 4:
            out = out + 4 - 8 * bit_y
        return out

    def flipped(flip_y, flip_x, flip_c):
        return ((bit_y + flip_y) % 2) * 4 + ((bit_x + flip_x) % 2) * 2 + (bit_c + flip_c) % 2

    def rows(idx):
        return pl.ds(pl.multiple_of(idx * part, part), part)

    def sub_rows(idx, sub):
        return pl.ds(pl.multiple_of(idx * part + sub * small, small), small)

    def slice_at(blk, slot, arr, where):
        if slot == 3:
            return g_out[blk].at[where, :]
        return (xg, gg)[arr].at[blk, slot, where, :]

    def buf_part(blk, slot, arr, mask, sub):
        return slice_at(blk, slot, arr, sub_rows(ident(mask), sub))

    def buf_slice(blk, slot, arr, mask):
        return slice_at(blk, slot, arr, rows(ident(mask)))

    def recv_at(blk, slot, arr, mask, sub=0):
        return recv.at[(((blk * 4 + slot) * 2 + arr) * 8 + mask) * SUB + sub]

    sent = []

    def remote(src, dst, where, rsem, cond=None):
        idx = len(sent)

        def make():
            return pltpu.make_async_remote_copy(src_ref=src(), dst_ref=dst(), send_sem=send.at[idx], recv_sem=rsem(), device_id=where(), device_id_type=MESH)

        sent.append((make, cond))
        if cond is None:
            make().start()
        else:
            pl.when(cond())(lambda: make().start())

    def wait_on(here, sem):
        pltpu.make_async_copy(here, here, sem).wait()

    def forward(blk, slot, arr, mask, sub, flip):
        here = lambda: buf_part(blk, slot, arr, mask, sub)
        remote(here, here, lambda: (z, ident(flip)), lambda: recv_at(blk, slot, arr, mask ^ flip, sub))

    def to_partner(blk, slot, arr, mask):
        here = lambda: buf_slice(blk, slot, arr, mask)
        remote(here, here, lambda: (z, ident(1)), lambda: recv_at(blk, slot, arr, mask ^ 1))

    def direct(blk, slot, arr):
        return "d" in ROUTE[blk, slot, arr][0]

    def is_end():
        return z % 3 == 0

    def is_inner():
        return z % 3 != 0

    def toward_middle():
        return z + 1 - 2 * (z // 2)

    def toward_end():
        return (z - 1 + 2 * (z // 2)) % N_DP

    def z_copy(src, blk, slot, arr, mask, sub, dest, cond):
        if mask == 0 or direct(blk, slot, arr):
            remote(src, lambda: buf_part(blk, slot, arr, mask, sub), lambda: (dest(), p), lambda: recv_at(blk, slot, arr, mask, sub), cond)

    def z_send(blk, arr, mask, sub):
        def src():
            whole = x_sv.at[blk] if arr == 0 else (g_in if blk == 1 else g_1)
            return whole.at[sub_rows(ident(mask), sub), :]

        z_copy(src, blk, 0, arr, mask, sub, toward_end, is_inner)
        z_copy(src, blk, 0, arr, mask, sub, toward_middle, is_end)
        z_copy(src, blk, 1, arr, mask, sub, toward_middle, is_inner)

    def send_on(blk, slot, arr, mask, sub):
        first, second = (2, 4) if "x" in ROUTE[blk, slot, arr][0] else (4, 2)
        if slot < 3 and mask in (0, 6):
            where = (2, toward_middle) if slot == 0 else (slot, toward_end)
            z_copy(lambda: buf_part(blk, slot, arr, mask, sub), blk, where[0], arr, mask, sub, where[1], is_inner)
        if mask == 0:
            forward(blk, slot, arr, 0, sub, first)
            forward(blk, slot, arr, 0, sub, second)
        elif mask == first and not direct(blk, slot, arr):
            forward(blk, slot, arr, first, sub, second)
        if sub == SUB - 1:
            to_partner(blk, slot, arr, mask)
        if (blk, slot, mask) == (1, 3, 6):
            z_send(0, 1, 6, sub)

    def halves(half):
        return pl.ds(half * part, part)

    def fetch(arr, step, dst, sem):
        at = step % HALF
        blk = 1 - step // HALF

        @pl.when(at < OWN)
        def _():
            for half in range(2):
                idx = flipped(at // 2, at % 2, half)
                if arr == 0:
                    pltpu.make_async_copy(x_sv.at[blk, rows(idx), :], dst(half), sem(half)).start()
                else:
                    @pl.when(blk == 1)
                    def _():
                        pltpu.make_async_copy(g_in.at[rows(idx), :], dst(half), sem(half)).start()

                    @pl.when(blk == 0)
                    def _():
                        here = g_1.at[rows(idx), :]
                        if half == 1:
                            wait_on(here, recv_at(1, 3, 1, 2 * at + 1))
                        pltpu.make_async_copy(here, dst(half), sem(half)).start()

        @pl.when(at >= OWN)
        def _():
            slot = (at - OWN) // 4
            quarter = (at - OWN) % 4
            buf = (xg, gg)[arr]
            for half in range(2):
                here = buf.at[blk, slot, rows(flipped(quarter // 2, half, quarter % 2)), :]

                @pl.when(quarter % 2 == 1)
                def _():
                    wait_on(here, recv_at(blk, slot, arr, 1 + 4 * (quarter // 2) + 2 * half))

                pltpu.make_async_copy(here, dst(half), sem(half)).start()

    def x_dst(step):
        slot = step % 2
        return (lambda half: xb.at[slot, halves(half), :]), (lambda half: x_sem.at[slot * 2 + half])

    def g_dst():
        return (lambda half: gb.at[halves(half), :]), (lambda half: g_sem.at[half])

    def fetched(dst, sem):
        for half in range(2):
            wait_on(dst(half), sem(half))

    def h_fetch(step):
        at = step % HALF
        for half in range(2):
            pltpu.make_async_copy(h_sv.at[1 - step // HALF, rows(flipped(at // 2, at % 2, half)), :], hb.at[halves(half), :], h_sem.at[half]).start()

    def pair_copy(blk, at):
        return pltpu.make_async_remote_copy(src_ref=pst.at[halves(1), :], dst_ref=pcb.at[at % 2], send_sem=misc.at[0], recv_sem=rs_pc.at[blk * OWN + at], device_id=(z, ident(1)), device_id_type=MESH)

    chunk = 16

    def pair_sum(blk, at):
        wait_on(pcb.at[at % 2], rs_pc.at[blk * OWN + at])
        pair_copy(blk, at).wait_send()

        def add(r, carry):
            where = pl.ds(pl.multiple_of(r * chunk, chunk), chunk)
            pst[where, :] = (pst[where, :].astype(F32) + pcb[at % 2, where, :].astype(F32)).astype(BF)
            return carry

        lax.fori_loop(0, part // chunk, add, 0)
        copy = pltpu.make_async_copy(pst.at[halves(0), :], pair.at[blk, at], misc.at[1])
        copy.start()
        copy.wait()
        if at == 1:
            p_send(blk, 1, 0, 0, 0)
        if at == 2:
            p_send(blk, 2, 1, 1, 1)
        if at == 3:
            p_send(blk, 3, 0, 2, 0)
            p_send(blk, 3, 1, 2, 1)

    def half_rows(low):
        return pl.ds(low * (part // 2), part // 2)

    def p_send(blk, src, low, dst, axis):
        remote(lambda: pair.at[blk, src, half_rows(low), :], lambda: rsr.at[blk, dst, half_rows(low), :], lambda: (z, ident(2 + 2 * axis)), lambda: rs_own.at[blk * 6 + dst * 2 + low])

    def p_wait(blk, dst):
        for low in range(2):
            wait_on(rsr.at[blk, dst, half_rows(low), :], rs_own.at[blk * 6 + dst * 2 + low])

    def run_copies(copies):
        for copy in copies:
            copy.start()
        for copy in copies:
            copy.wait()

    def combine(blk):
        p_wait(blk, 2)
        run_copies([
            pltpu.make_async_copy(pair.at[blk, 2, half_rows(0), :], pst.at[half_rows(0), :], misc.at[1]),
            pltpu.make_async_copy(pair.at[blk, 1, half_rows(1), :], pst.at[half_rows(1), :], misc.at[2]),
            pltpu.make_async_copy(rsr.at[blk, 2], pcb.at[0], misc.at[3]),
        ])

        def add(r, carry):
            lo = pl.ds(pl.multiple_of(r * chunk, chunk), chunk)
            pst[lo, :] = (pst[lo, :].astype(F32) + pcb[0, lo, :].astype(F32)).astype(BF)
            return carry

        lax.fori_loop(0, part // chunk, add, 0)
        run_copies([
            pltpu.make_async_copy(pst.at[half_rows(0), :], pair.at[blk, 2, half_rows(0), :], misc.at[1]),
            pltpu.make_async_copy(pst.at[half_rows(1), :], pair.at[blk, 1, half_rows(1), :], misc.at[2]),
        ])
        p_send(blk, 2, 0, 1, 1)
        p_send(blk, 1, 1, 0, 0)

    def reduce_own(blk):
        p_wait(blk, 0)
        p_wait(blk, 1)
        before = g_in if blk == 1 else g_1
        run_copies([
            pltpu.make_async_copy(pair.at[blk, 0], pst.at[halves(0), :], misc.at[1]),
            pltpu.make_async_copy(rsr.at[blk, 0], pst.at[halves(1), :], misc.at[2]),
            pltpu.make_async_copy(rsr.at[blk, 1], pcb.at[0], misc.at[3]),
            pltpu.make_async_copy(before.at[rows(p), :], gb.at[halves(0), :], misc.at[5]),
        ])

        def add(r, carry):
            lo = pl.ds(pl.multiple_of(r * chunk, chunk), chunk)
            hi = pl.ds(pl.multiple_of(part + r * chunk, chunk), chunk)
            total = pst[lo, :].astype(F32) + pst[hi, :].astype(F32) + pcb[0, lo, :].astype(F32)
            pst[lo, :] = (gb[lo, :].astype(F32) + total).astype(BF)
            return carry

        lax.fori_loop(0, part // chunk, add, 0)
        run_copies([pltpu.make_async_copy(pst.at[halves(0), :], g_out[blk].at[rows(p), :], misc.at[1])])
        for sub in range(SUB):
            send_on(blk, 3, 1, 0, sub)
        if blk == 1:
            for sub in range(SUB):
                z_send(0, 1, 0, sub)

    def ticks(step, point):
        for blk in (1, 0):
            for when, act in ((COMBINE, combine), (REDUCE, reduce_own)):
                if when[blk] % 4 == point:
                    pl.when(step == when[blk] // 4)(functools.partial(act, blk))
        for mask, tick in zip((0, 6), X0_TICKS):
            if tick % 4 == point:
                @pl.when(step == tick // 4)
                def _(mask=mask):
                    for sub in range(SUB):
                        z_send(0, 0, mask, sub)
        for tick, evs in events_by_tick():
            if tick % 4 == point:
                @pl.when(step == tick // 4)
                def _(evs=evs):
                    for ev in evs:
                        wait_on(buf_part(*ev), recv_at(*ev))
                        send_on(*ev)

    def load_w1(blk):
        return pltpu.make_async_copy(w_up.at[blk], w1, misc.at[2])

    def load_w2(blk):
        return pltpu.make_async_copy(w_dn.at[blk], w2, misc.at[3])

    def store_1(blk):
        return pltpu.make_async_copy(acc1, dw1.at[blk], misc.at[4])

    def store_2(blk):
        return pltpu.make_async_copy(acc2, dw2.at[blk], misc.at[5])

    def clear(ref):
        def some(r, carry):
            ref[pl.ds(pl.multiple_of(r * 16, 16), 16), :] = jnp.zeros((16, ref.shape[1]), F32)
            return carry

        lax.fori_loop(0, ref.shape[0] // 16, some, 0)

    load_w2(1).start()
    fetch(1, 0, *g_dst())
    h_fetch(0)
    fetch(0, 0, *x_dst(0))
    load_w1(1).start()
    for arr, mask in Z_ORDER:
        for sub in range(SUB):
            z_send(1, arr, mask, sub)
    clear(acc2)
    clear(acc1)
    load_w2(1).wait()
    load_w1(1).wait()

    n_hid = 256
    n_dim = 512

    def hid_cols(j):
        return pl.ds(pl.multiple_of(j * n_hid, n_hid), n_hid)

    def dim_cols(j):
        return pl.ds(pl.multiple_of(j * n_dim, n_dim), n_dim)

    def step_body(step, carry):
        slot = step % 2
        at = step % HALF
        is_own = at < OWN
        ticks(step, 0)
        fetched(*x_dst(step))

        @pl.when(is_own)
        def _():
            for half in range(2):
                wait_on(hb.at[halves(half), :], h_sem.at[half])

        @pl.when(at >= OWN)
        def _():
            def h_part(j, c):
                hb[:, hid_cols(j)] = dot_nn(xb[slot], w1[:, hid_cols(j)]).astype(BF)
                return c

            lax.fori_loop(0, hid // n_hid, h_part, 0, unroll=True)

        ticks(step, 1)

        @pl.when(step == HALF - 1)
        def _():
            load_w1(0).start()

        @pl.when(step == HALF)
        def _():
            store_2(1).wait()
            clear(acc2)
            load_w2(0).wait()

        fetched(*g_dst())

        def a_part(j, c):
            act, slope = gelu_parts(hb[:, hid_cols(j)].astype(F32))
            ab[:, hid_cols(j)] = act.astype(BF)
            dhb[:, hid_cols(j)] = (dot_nt(gb[...], w2[hid_cols(j), :]) * slope).astype(BF)
            return c

        lax.fori_loop(0, hid // n_hid, a_part, 0, unroll=True)

        def down_part(j, c):
            acc2[hid_cols(j), :] += dot_tn(ab[:, hid_cols(j)], gb[...])
            return c

        lax.fori_loop(0, hid // n_hid, down_part, 0, unroll=True)

        @pl.when(step == HALF - 1)
        def _():
            load_w2(0).start()
            store_2(1).start()

        @pl.when(step == STEPS - 1)
        def _():
            store_2(0).start()

        ticks(step, 2)

        @pl.when(step + 1 < STEPS)
        def _():
            fetch(0, step + 1, *x_dst(step + 1))
            fetch(1, step + 1, *g_dst())

        @pl.when((step + 1) % HALF < OWN)
        def _():
            pl.when(step + 1 < STEPS)(lambda: h_fetch(step + 1))

        for blk in (1, 0):
            for b in range(OWN):
                pl.when(step == (1 - blk) * HALF + b + 1)(functools.partial(pair_sum, blk, b))

        @pl.when(step == HALF)
        def _():
            load_w1(0).wait()

        @pl.when(is_own)
        def _():
            def p_part(j, c):
                pst[:, dim_cols(j)] = dot_nt(dhb[...], w1[dim_cols(j), :]).astype(BF)
                return c

            lax.fori_loop(0, dim // n_dim, p_part, 0, unroll=True)

        ticks(step, 3)
        for blk in (1, 0):
            for b in range(OWN):
                pl.when(step == (1 - blk) * HALF + b)(lambda blk=blk, b=b: pair_copy(blk, b).start())

        @pl.when(step == HALF)
        def _():
            store_1(1).wait()
            clear(acc1)

        def up_part(j, c):
            acc1[dim_cols(j), :] += dot_tn(xb[slot, :, dim_cols(j)], dhb[...])
            return c

        @pl.when(step < STEPS - 1)
        def _():
            lax.fori_loop(0, dim // n_dim, up_part, 0, unroll=True)

        @pl.when(step == HALF - 1)
        def _():
            store_1(1).start()

        return carry

    lax.fori_loop(0, STEPS, step_body, 0)

    def last_part(j):
        return pltpu.make_async_copy(acc1.at[dim_cols(j), :], dw1.at[0, dim_cols(j), :], misc.at[4])

    def last_up(j, c):
        acc1[dim_cols(j), :] += dot_tn(xb[(STEPS - 1) % 2, :, dim_cols(j)], dhb[...])

        @pl.when(j > 0)
        def _():
            last_part(j - 1).wait()

        last_part(j).start()
        return c

    lax.fori_loop(0, dim // n_dim, last_up, 0)
    last_part(dim // n_dim - 1).wait()
    for mask in (1, 3, 5, 7):
        wait_on(buf_slice(0, 3, 1, mask), recv_at(0, 3, 1, mask))
    for make, cond in sent:
        if cond is None:
            make().wait_send()
        else:
            pl.when(cond())(lambda make=make: make().wait_send())
    store_2(0).wait()


def backward(w_up, w_dn, x_sv, h_sv, g_in):
    _, dim, hid = w_up.shape
    tokens = g_in.shape[0]
    part = tokens // N_TP
    hbm = pl.BlockSpec(memory_space=pl.ANY)
    outs = [
        jax.ShapeDtypeStruct((tokens, dim), BF),
        jax.ShapeDtypeStruct((tokens, dim), BF),
        jax.ShapeDtypeStruct((2, dim, hid), F32),
        jax.ShapeDtypeStruct((2, hid, dim), F32),
        jax.ShapeDtypeStruct((2, 3, tokens, dim), BF),
        jax.ShapeDtypeStruct((2, 3, tokens, dim), BF),
        jax.ShapeDtypeStruct((2, 3, part, dim), BF),
        jax.ShapeDtypeStruct((2, 4, part, dim), BF),
    ]
    dma = pltpu.SemaphoreType.DMA
    scratch = [
        pltpu.VMEM((dim, hid), BF),
        pltpu.VMEM((hid, dim), BF),
        pltpu.VMEM((dim, hid), F32),
        pltpu.VMEM((hid, dim), F32),
        pltpu.VMEM((2, 2 * part, dim), BF),
        pltpu.VMEM((2 * part, dim), BF),
        pltpu.VMEM((2 * part, hid), BF),
        pltpu.VMEM((2 * part, hid), BF),
        pltpu.VMEM((2 * part, hid), BF),
        pltpu.VMEM((2 * part, dim), BF),
        pltpu.VMEM((2, part, dim), BF),
        dma((6,)),
        dma((4,)),
        dma((2,)),
        dma((2,)),
        dma((2 * OWN,)),
        dma((12,)),
        dma((256,)),
        dma((288,)),
    ]
    return pl.pallas_call(
        kernel,
        out_shape=outs,
        in_specs=[hbm] * 5,
        out_specs=[hbm] * len(outs),
        scratch_shapes=scratch,
        compiler_params=pltpu.CompilerParams(has_side_effects=True, vmem_limit_bytes=67043328),
        cost_estimate=pl.CostEstimate(flops=STEPS * 4 * 4 * part * dim * hid, bytes_accessed=0, transcendentals=0),
        name="backward",
    )(w_up, w_dn, x_sv, h_sv, g_in)


def solution(mesh):
    def run_backward(w_up, w_down, x_saved, h_saved, grad_out):
        grad_in, _, up, down, *_ = backward(w_up, w_down, x_saved[:, 0], h_saved[:, 0], grad_out[0])
        return grad_in[None], up, down

    return jax.shard_map(run_backward, mesh=mesh, in_specs=(P(None, None, "tp"), P(None, "tp", None), P(None, "dp", None, None), P(None, "dp", None, "tp"), P("dp", None, None)), out_specs=(P("dp", None, None), P(None, None, "tp"), P(None, "tp", None)), check_vma=False)
```
